32 devices in a mesh: tensor: 2 (over x), dp: 16 (over z, y, core).
Axes of the slice: x: 2, y: 2, z: 4, core: 2. Of those that a mesh axis runs over, the one named last changes fastest.
Arguments:
- tokens: bfloat16 [2048, 8192], P('dp', 'tensor'), may hold values from -6 to 6
- projection_weights: bfloat16 [2, 8192, 256], P(None, None, 'tensor'), may hold values from -0.0625 to 0.0625
- head_cotangent: bfloat16 [2, 2048, 256], P(None, 'dp', 'tensor'), may hold values from -6 to 6
- frequencies: int32 [2, 1024], replicated, may hold values from 0 to 8191, as said below
- sign_bits: int32 [2, 8192], replicated, may hold values 0 or 1
- first_moment: float32 [2, 1024, 256], P(None, 'dp', 'tensor'), may hold values from -6 to 6
- second_moment: float32 [2, 1024, 256], P(None, 'dp', 'tensor'), may hold values from 0.2 to 2
Outputs:
- input_gradient: bfloat16 [2048, 8192], P('dp', 'tensor')
- new_first: float32 [2, 1024, 256], P(None, 'dp', 'tensor')
- new_second: float32 [2, 1024, 256], P(None, 'dp', 'tensor')
- full_direction: bfloat16 [2, 8192, 256], P(None, 'dp', 'tensor')
The draws below stay inside these ranges and needn't reach their ends.
Inputs may be any that keep to these rules, and one draw needn't show every extreme that they name: Each row holds 1024 different frequencies, and 0 is one of them.
All inputs are finite; a program needn't handle non-finite values.
Results may differ from the reference program's by a relative error of at most 0.013.
Values may be sent and summed in bfloat16 or wider, within the bound.
A program may use at most 64 MiB of HBM per device.

```python
import math
import jax
import jax.numpy as jnp
from jax import lax

D = 8192
RANK = 1024
KV = 256
TOKENS = 2048
N_TENSOR = 2


def frequency_row(key, salt):
    chosen = jax.random.permutation(jax.random.fold_in(key, salt), D - 1)[:RANK] + 1
    position = jax.random.randint(jax.random.fold_in(key, salt + 100), (), 0, RANK)
    return chosen.at[position].set(0).astype(jnp.int32)


def draw_frequencies(key, part):
    return jnp.stack([frequency_row(key, 11), frequency_row(key, 12)]).astype(jnp.int32)


def set_ends(array, rng, smallest, high):
    shape = array.shape
    place = [jax.random.randint(jax.random.fold_in(rng, axis), (), 0, shape[axis]) for axis in range(len(shape))]
    array = array.at[tuple(place)].set(smallest)
    longest = shape.index(max(shape))
    place[longest] = (place[longest] + 1) % shape[longest]
    return array.at[tuple(place)].set(high)


def block_scale(key, dims, shards, least, top_value):
    def one(dim, shards_of):
        heights = jax.random.uniform(jax.random.fold_in(jax.random.fold_in(key, 6), dim), (shards_of,), jnp.float32, least / len(shards), top_value / len(shards))
        return jnp.repeat(jnp.exp(heights), dims[dim] // shards_of).reshape((-1,) + (1,) * (len(dims) - dim - 1))

    gain = one(*shards[0])
    for cut in shards[1:]:
        gain = gain * one(*cut)
    return gain


def centred(stream_key, shape, width, limit, split=(), kind=jnp.bfloat16):
    values = jax.random.normal(stream_key, shape, jnp.float32) * width
    if len(split) > 0:
        values = block_scale(stream_key, shape, split, -0.22, 0.18) * values
    return jnp.clip(values, min=-limit, max=limit).astype(kind)


def setup_inputs(seed: int = 0) -> dict:
    streams_of = jax.random.split(jax.random.key(seed), 8)
    return {
        "tokens": centred(streams_of[0], (TOKENS, D), 1.0, 6.0, ((0, 16), (1, 2))),
        "projection_weights": centred(streams_of[1], (2, D, KV), D ** -0.5, 0.0625, ((2, 2),)),
        "head_cotangent": centred(streams_of[2], (2, TOKENS, KV), 1.0, 6.0, ((1, 16), (2, 2))),
        "frequencies": draw_frequencies(jax.random.fold_in(streams_of[7], 71), 0),
        "sign_bits": set_ends((jax.random.randint(streams_of[4], (2, D), 0, 2) < 1).astype(jnp.int32), jax.random.fold_in(streams_of[4], 1), 0, 1),
        "first_moment": centred(streams_of[5], (2, RANK, KV), 1.0, 6.0, ((1, 16), (2, 2)), jnp.float32),
        "second_moment": jnp.clip(jnp.exp(math.log(2.0) - 2.3025851 * jax.random.uniform(streams_of[6], (2, RANK, KV), jnp.float32) ** block_scale(streams_of[6], (2, RANK, KV), ((1, 16), (2, 2)), -0.2, 0.2)), 0.2, 2.0),
    }


first_fix = 1.0 - 0.9 ** 10
second_fix = 1.0 - 0.95 ** 10
epsilon = 1e-08

def basis_rows(frequency, sign_part, offset, row_count, full_width):
    row_index = offset + lax.iota(jnp.int32, row_count)
    row_sign = lax.dynamic_slice_in_dim(sign_part, offset, row_count, 0)
    phase_index = (2 * row_index[:, None] + 1) * frequency[None, :] % (4 * full_width)
    angles = phase_index.astype(jnp.float32) * (math.pi / (2 * full_width))
    column_scale = jnp.where(frequency == 0, math.sqrt(1.0 / full_width), math.sqrt(2.0 / full_width)).astype(jnp.float32)
    signed = (2 * row_sign - 1).astype(jnp.float32)
    return (jnp.cos(angles) * column_scale[None, :] * signed[:, None]).astype(jnp.bfloat16)

def adam_update(gradient, first_moment, second_moment):
    new_first = 0.9 * first_moment + 0.1 * gradient
    new_second = 0.95 * second_moment + 0.05 * gradient * gradient
    direction = (new_first / first_fix / (jnp.sqrt(new_second / second_fix) + epsilon)).astype(jnp.bfloat16)
    return (new_first, new_second, direction)

def reference(tokens, projection_weights, head_cotangent, frequencies, sign_bits, first_moment, second_moment):
    token_count, full_width = tokens.shape
    head_width = projection_weights.shape[2] // N_TENSOR
    bases = [basis_rows(frequencies[matrix], sign_bits[matrix], 0, full_width, full_width) for matrix in range(2)]
    gradients = []
    for matrix in range(2):
        projected = jnp.dot(tokens, bases[matrix], preferred_element_type=jnp.float32).astype(jnp.bfloat16)
        low_rank = jnp.dot(projected.T, head_cotangent[matrix], preferred_element_type=jnp.float32)
        gradients.append(low_rank / math.sqrt(token_count))
    gradient = jnp.stack(gradients)
    new_first, new_second, direction = adam_update(gradient, first_moment, second_moment)
    full_direction = jnp.stack([jnp.dot(bases[matrix], direction[matrix], preferred_element_type=jnp.float32) for matrix in range(2)]).astype(jnp.bfloat16)
    summed = jnp.zeros((token_count, full_width), jnp.float32)
    for tensor_rank in range(N_TENSOR):
        columns = slice(tensor_rank * head_width, (tensor_rank + 1) * head_width)
        partial_sum = jnp.dot(head_cotangent[0][:, columns], projection_weights[0][:, columns].T, preferred_element_type=jnp.float32)
        partial_sum = partial_sum + jnp.dot(head_cotangent[1][:, columns], projection_weights[1][:, columns].T, preferred_element_type=jnp.float32)
        rounded = lax.optimization_barrier(partial_sum.astype(jnp.bfloat16))
        summed = summed + rounded.astype(jnp.float32)
    return (summed.astype(jnp.bfloat16), new_first, new_second, full_direction)
```

```python
import functools
import math

import jax
import jax.numpy as jnp
from jax import lax
from jax.experimental import pallas as pl
from jax.experimental.pallas import tpu as pltpu
from jax.sharding import PartitionSpec as P

first_fix = 1.0 - 0.9**10
second_fix = 1.0 - 0.95**10
epsilon = 1e-08


def trig(phase, width):
    phase = phase % (4 * width)
    quarter = (phase + width // 2) // width
    x = (phase - quarter * width).astype(jnp.float32) * (math.pi / (2 * width))
    y = x * x
    c = 1.0 + y * (-0.5 + y * (1 / 24 + y * (-1 / 720 + y * (1 / 40320 - y * (1 / 3628800)))))
    s = x * (1.0 + y * (-1 / 6 + y * (1 / 120 + y * (-1 / 5040 + y * (1 / 362880)))))
    quarter = quarter % 4
    odd = quarter % 2 == 1
    cosine = jnp.where(odd, s, c) * jnp.where((quarter == 1) | (quarter == 2), -1.0, 1.0)
    sine = jnp.where(odd, c, s) * jnp.where(quarter >= 2, -1.0, 1.0)
    return cosine, sine


def project_kernel(low_rows, chunk, tok_ref, hc_ref, sign_ref, ca_ref, sa_ref, cb_ref, sb_ref, out_ref, acc):
    rank = acc.shape[2]
    groups = chunk // low_rows
    dp, n_tensor, _, own, cols = out_ref.shape
    acc[...] = jnp.zeros_like(acc)

    def step(h, carry):
        columns = pl.ds(pl.multiple_of(h * chunk, chunk), chunk)
        tok = tok_ref[:, columns]
        for m in range(2):
            ks = slice(m * rank, (m + 1) * rank)
            cb, sb = cb_ref[:, ks], sb_ref[:, ks]
            parts = []
            for g in range(groups):
                row = pl.ds(h * groups + g, 1)
                parts.append((ca_ref[row, ks] * cb - sa_ref[row, ks] * sb).astype(jnp.bfloat16))
            basis = jnp.concatenate(parts, axis=0) if groups > 1 else parts[0]
            signed = tok * sign_ref[pl.ds(m, 1), columns].astype(jnp.bfloat16)
            acc[m] += jnp.dot(signed, basis, preferred_element_type=jnp.float32)
        return carry

    lax.fori_loop(0, tok_ref.shape[1] // chunk, step, 0)
    for m in range(2):
        low = lax.dot_general(
            acc[m].astype(jnp.bfloat16),
            hc_ref[m],
            (((0,), (0,)), ((), ())),
            preferred_element_type=jnp.float32,
        ).astype(jnp.bfloat16)
        for t in range(n_tensor):
            out_ref[:, t, m] = low[:, t * cols : (t + 1) * cols].reshape(dp, own, cols)


def shards(
    tokens, projection_weights, head_cotangent, frequencies, sign_bits, first_moment, second_moment
):
    rows, local_width = tokens.shape
    n_tensor, n_dp = lax.axis_size("tensor"), lax.axis_size("dp")
    width = local_width * n_tensor
    token_count = rows * n_dp
    rank = frequencies.shape[1]
    own, cols = first_moment.shape[1], first_moment.shape[2]
    own_rows = projection_weights.shape[1] // n_dp
    low_rows = min(128, own_rows)
    chunk = min(256, local_width)
    me_t, me_d = lax.axis_index("tensor"), lax.axis_index("dp")
    offset = me_t * local_width
    row_offset = me_d * own_rows

    head_contract = (((1,), (1,)), ((), ()))

    def partial(t):
        total = 0.0
        for m in range(2):
            w = lax.dynamic_slice_in_dim(projection_weights[m], t * local_width, local_width, 0)
            total = total + lax.dot_general(
                head_cotangent[m], w, head_contract, preferred_element_type=jnp.float32
            )
        return total.astype(jnp.bfloat16)

    arrived = []
    for shift in range(1, n_tensor):
        sent = partial((me_t + shift) % n_tensor)
        pairs = [(i, (i + shift) % n_tensor) for i in range(n_tensor)]
        arrived.append(lax.ppermute(sent, "tensor", pairs))
    mine = partial(me_t)
    heads = lax.all_gather(head_cotangent, "tensor", axis=2, tiled=True)

    f = frequencies.reshape(1, 2 * rank)
    scale = jnp.where(f == 0, math.sqrt(1.0 / width), math.sqrt(2.0 / width)).astype(jnp.float32)
    cb, sb = trig((2 * lax.iota(jnp.int32, low_rows)[:, None] + 1) * f, width)
    hi = offset + low_rows * lax.iota(jnp.int32, local_width // low_rows)
    ca, sa = trig(2 * hi[:, None] * f, width)
    ca, sa = ca * scale, sa * scale
    hi_b = row_offset + low_rows * lax.iota(jnp.int32, own_rows // low_rows)
    ra, rb = trig(2 * hi_b[:, None] * f, width)
    ra, rb = ra * scale, rb * scale
    signs = (2 * sign_bits - 1).astype(jnp.float32)
    my_signs = lax.dynamic_slice_in_dim(signs, offset, local_width, 1)

    vmem = pl.BlockSpec(memory_space=pltpu.VMEM)
    low = pl.pallas_call(
        functools.partial(project_kernel, low_rows, chunk),
        out_shape=jax.ShapeDtypeStruct((n_dp, n_tensor, 2, own, cols), jnp.bfloat16),
        in_specs=[vmem] * 7,
        out_specs=vmem,
        scratch_shapes=[pltpu.VMEM((2, rows, rank), jnp.float32)],
        compiler_params=pltpu.CompilerParams(vmem_limit_bytes=32 * 1024 * 1024),
        cost_estimate=pl.CostEstimate(
            flops=4 * rows * local_width * rank * 4, bytes_accessed=8 * 2**20, transcendentals=0
        ),
    )(tokens, heads, my_signs, ca, sa, cb, sb)
    pieces = lax.all_to_all(
        low.reshape(n_dp * n_tensor, 2, own, cols), ("dp", "tensor"), 0, 0, tiled=True
    )
    gradient = jnp.sum(pieces.astype(jnp.float32), axis=0) / math.sqrt(token_count)
    new_first = 0.9 * first_moment + 0.1 * gradient
    new_second = 0.95 * second_moment + 0.05 * gradient * gradient
    direction = (new_first / first_fix / (jnp.sqrt(new_second / second_fix) + epsilon)).astype(
        jnp.bfloat16
    )
    gathered = lax.all_gather(direction, "dp", axis=1, tiled=True)
    back = []
    for m in range(2):
        ks = slice(m * rank, (m + 1) * rank)
        basis = ra[:, None, ks] * cb[None, :, ks] - rb[:, None, ks] * sb[None, :, ks]
        row_sign = lax.dynamic_slice_in_dim(signs[m], row_offset, own_rows, 0)[:, None]
        basis = basis.reshape(own_rows, rank).astype(jnp.bfloat16)
        product = jnp.dot(basis, gathered[m], preferred_element_type=jnp.float32)
        back.append((product * row_sign).astype(jnp.bfloat16))
    summed = mine.astype(jnp.float32)
    for piece in arrived:
        summed = summed + piece.astype(jnp.float32)
    return (summed.astype(jnp.bfloat16), new_first, new_second, jnp.stack(back))


def solution(mesh):
    in_specs = (
        P("dp", "tensor"),
        P(None, None, "tensor"),
        P(None, "dp", "tensor"),
        P(),
        P(),
        P(None, "dp", "tensor"),
        P(None, "dp", "tensor"),
    )
    out_specs = (
        P("dp", "tensor"),
        P(None, "dp", "tensor"),
        P(None, "dp", "tensor"),
        P(None, "dp", "tensor"),
    )
    return jax.shard_map(shards, mesh=mesh, in_specs=in_specs, out_specs=out_specs, check_vma=False)
```

```python
import functools
import math

import jax
import jax.numpy as jnp
from jax import lax
from jax.experimental import pallas as pl
from jax.experimental.pallas import tpu as pltpu
from jax.sharding import PartitionSpec as P

first_fix = 1.0 - 0.9**10
second_fix = 1.0 - 0.95**10
epsilon = 1e-08


def trig(phase, width):
    phase = phase % (4 * width)
    quarter = (phase + width // 2) // width
    x = (phase - quarter * width).astype(jnp.float32) * (math.pi / (2 * width))
    y = x * x
    c = 1.0 + y * (-0.5 + y * (1 / 24 + y * (-1 / 720 + y * (1 / 40320 - y * (1 / 3628800)))))
    s = x * (1.0 + y * (-1 / 6 + y * (1 / 120 + y * (-1 / 5040 + y * (1 / 362880)))))
    quarter = quarter % 4
    odd = quarter % 2 == 1
    cosine = jnp.where(odd, s, c) * jnp.where((quarter == 1) | (quarter == 2), -1.0, 1.0)
    sine = jnp.where(odd, c, s) * jnp.where(quarter >= 2, -1.0, 1.0)
    return cosine, sine


def step_kernel(
    low_rows, chunk, token_count,
    tok_ref, w_ref, hc_ref, sign_ref, back_sign_ref, ca_ref, sa_ref, cb_ref, sb_ref, ra_ref, rb_ref,
    first_ref, second_ref,
    grad_ref, new_first_ref, new_second_ref, full_ref,
    acc, hc_all, tg_send, tg_recv, low_send, low_recv, part, x_send, x_recv, dirs, back_basis,
    hc_sems, tg_sems, low_sems, x_sems, dir_sems,
):
    rank = acc.shape[2]
    rows, lw = tok_ref.shape
    groups = chunk // low_rows
    n_dp, n_t, _, own, cols = low_send.shape
    me_t, me_d = lax.axis_index("tensor"), lax.axis_index("dp")

    def remote(src, dst, sems, slot, tensor, dp):
        return pltpu.make_async_remote_copy(
            src_ref=src,
            dst_ref=dst,
            send_sem=sems.at[0, slot],
            recv_sem=sems.at[1, slot],
            device_id={"tensor": tensor, "dp": dp},
            device_id_type=pl.DeviceIdType.MESH,
        )

    def peer_t(s):
        return lax.rem(me_t + s, n_t)

    def peer_d(s):
        return lax.rem(me_d + s, n_dp)

    barrier = pltpu.get_barrier_semaphore()

    def greet_t(s, carry):
        pl.semaphore_signal(
            barrier, inc=1, device_id={"tensor": peer_t(s), "dp": me_d},
            device_id_type=pl.DeviceIdType.MESH,
        )
        return carry

    def greet_d(s, carry):
        pl.semaphore_signal(
            barrier, inc=1, device_id={"tensor": me_t, "dp": peer_d(s)},
            device_id_type=pl.DeviceIdType.MESH,
        )
        return carry

    lax.fori_loop(1, n_t, greet_t, 0)
    lax.fori_loop(1, n_dp, greet_d, 0)
    pl.semaphore_wait(barrier, n_t + n_dp - 2)

    def hc_copy(s):
        return remote(hc_ref, hc_all.at[me_t], hc_sems, s, peer_t(s), me_d)

    def tg_copy(s):
        return remote(tg_send.at[s - 1], tg_recv.at[s - 1], tg_sems, s, peer_t(s), me_d)

    def low_copy(s):
        return remote(low_send.at[peer_d(s)], low_recv.at[s - 1], low_sems, s, me_t, peer_d(s))

    def x_copy(s):
        return remote(x_send.at[peer_t(s)], x_recv.at[s - 1], x_sems, s, peer_t(s), me_d)

    def dir_copy(s):
        return remote(dirs.at[me_d], dirs.at[me_d], dir_sems, s, me_t, peer_d(s))

    def each(count, act):
        def body(s, carry):
            act(s)
            return carry

        lax.fori_loop(1, count, body, 0)

    each(n_t, lambda s: hc_copy(s).start())
    hc_all[pl.ds(me_t, 1)] = hc_ref[...][None]
    wide = min(512, lw)

    def partial(t, j):
        total = 0.0
        for m in range(2):
            w = w_ref[m, pl.ds(pl.multiple_of(t * lw + j * wide, wide), wide), :]
            total = total + lax.dot_general(
                hc_ref[m], w, (((1,), (1,)), ((), ())), preferred_element_type=jnp.float32
            )
        return total.astype(jnp.bfloat16)

    def send_half(s):
        def tile(j, carry):
            tg_send[s - 1, :, pl.ds(pl.multiple_of(j * wide, wide), wide)] = partial(peer_t(s), j)
            return carry

        lax.fori_loop(0, lw // wide, tile, 0)
        tg_copy(s).start()

    each(n_t, send_half)
    acc[...] = jnp.zeros_like(acc)

    def tables(a_ref, b_ref, row, ks):
        row = pl.ds(row, 1)
        return (a_ref[row, ks] * cb_ref[:, ks] - b_ref[row, ks] * sb_ref[:, ks]).astype(jnp.bfloat16)

    def step(h, carry):
        columns = pl.ds(pl.multiple_of(h * chunk, chunk), chunk)
        tok = tok_ref[:, columns]
        for m in range(2):
            ks = slice(m * rank, (m + 1) * rank)
            parts = [tables(ca_ref, sa_ref, h * groups + g, ks) for g in range(groups)]
            basis = jnp.concatenate(parts, axis=0) if groups > 1 else parts[0]
            signed = tok * sign_ref[pl.ds(m, 1), columns].astype(jnp.bfloat16)
            acc[m] += jnp.dot(signed, basis, preferred_element_type=jnp.float32)
        return carry

    lax.fori_loop(0, lw // chunk, step, 0)
    each(n_t, lambda s: hc_copy(s).wait_recv())
    for m in range(2):
        heads = jnp.concatenate([hc_all[t, m] for t in range(n_t)], axis=1)
        low = lax.dot_general(
            acc[m].astype(jnp.bfloat16),
            heads,
            (((0,), (0,)), ((), ())),
            preferred_element_type=jnp.float32,
        ).astype(jnp.bfloat16)
        for t in range(n_t):
            low_send[:, t, m] = low[:, t * cols : (t + 1) * cols].reshape(n_dp, own, cols)
    each(n_dp, lambda s: low_copy(s).start())

    def own_tile(j, carry):
        grad_ref[:, pl.ds(pl.multiple_of(j * wide, wide), wide)] = partial(me_t, j)
        return carry

    lax.fori_loop(0, lw // wide, own_tile, 0)

    def back_rows(h, carry):
        for m in range(2):
            ks = slice(m * rank, (m + 1) * rank)
            place = pl.ds(pl.multiple_of(h * low_rows, low_rows), low_rows)
            back_basis[m, place, :] = tables(ra_ref, rb_ref, h, ks)
        return carry

    lax.fori_loop(0, back_basis.shape[1] // low_rows, back_rows, 0)
    part[...] = low_send[pl.ds(me_d, 1)][0].astype(jnp.float32)

    def add(s):
        low_copy(s).wait_recv()
        part[...] += low_recv[pl.ds(s - 1, 1)][0].astype(jnp.float32)

    each(n_dp, add)
    x_send[...] = part[...].astype(jnp.bfloat16)
    each(n_t, lambda s: x_copy(s).start())
    total = part[pl.ds(me_t, 1)][0]
    each(n_t, lambda s: x_copy(s).wait_recv())
    for s in range(1, n_t):
        total = total + x_recv[s - 1].astype(jnp.float32)
    gradient = total / math.sqrt(token_count)
    new_first = 0.9 * first_ref[...] + 0.1 * gradient
    new_second = 0.95 * second_ref[...] + 0.05 * gradient * gradient
    direction = new_first / first_fix / (jnp.sqrt(new_second / second_fix) + epsilon)
    dirs[pl.ds(me_d, 1)] = direction.astype(jnp.bfloat16)[None]
    each(n_dp, lambda s: dir_copy(s).start())
    new_first_ref[...] = new_first
    new_second_ref[...] = new_second
    each(n_t, lambda s: tg_copy(s).wait_recv())

    def finish(j, carry):
        place = pl.ds(pl.multiple_of(j * wide, wide), wide)
        summed = grad_ref[:, place].astype(jnp.float32)
        for s in range(1, n_t):
            summed = summed + tg_recv[s - 1, :, place].astype(jnp.float32)
        grad_ref[:, place] = summed.astype(jnp.bfloat16)
        return carry

    lax.fori_loop(0, lw // wide, finish, 0)

    def dir_arrival(s):
        source = lax.rem(me_d + n_dp - s, n_dp)
        remote(dirs.at[source], dirs.at[source], dir_sems, s, me_t, source).wait_recv()

    each(n_dp, dir_arrival)
    for m in range(2):
        product = jnp.dot(
            back_basis[m],
            dirs[:, m].reshape(rank, cols),
            preferred_element_type=jnp.float32,
        )
        full_ref[m] = (product * back_sign_ref[m]).astype(jnp.bfloat16)
    each(n_t, lambda s: hc_copy(s).wait_send())
    each(n_t, lambda s: tg_copy(s).wait_send())
    each(n_dp, lambda s: low_copy(s).wait_send())
    each(n_t, lambda s: x_copy(s).wait_send())
    each(n_dp, lambda s: dir_copy(s).wait_send())


def shards(
    tokens, projection_weights, head_cotangent, frequencies, sign_bits, first_moment, second_moment
):
    rows, local_width = tokens.shape
    n_tensor, n_dp = lax.axis_size("tensor"), lax.axis_size("dp")
    width = local_width * n_tensor
    token_count = rows * n_dp
    rank = frequencies.shape[1]
    own, cols = first_moment.shape[1], first_moment.shape[2]
    own_rows = projection_weights.shape[1] // n_dp
    low_rows = min(128, own_rows)
    chunk = min(256, local_width)
    me_t, me_d = lax.axis_index("tensor"), lax.axis_index("dp")
    offset = me_t * local_width
    row_offset = me_d * own_rows

    f = frequencies.reshape(1, 2 * rank)
    scale = jnp.where(f == 0, math.sqrt(1.0 / width), math.sqrt(2.0 / width)).astype(jnp.float32)
    cb, sb = trig((2 * lax.iota(jnp.int32, low_rows)[:, None] + 1) * f, width)
    hi = offset + low_rows * lax.iota(jnp.int32, local_width // low_rows)
    ca, sa = trig(2 * hi[:, None] * f, width)
    ca, sa = ca * scale, sa * scale
    hi_b = row_offset + low_rows * lax.iota(jnp.int32, own_rows // low_rows)
    ra, rb = trig(2 * hi_b[:, None] * f, width)
    ra, rb = ra * scale, rb * scale
    signs = (2 * sign_bits - 1).astype(jnp.float32)
    my_signs = lax.dynamic_slice_in_dim(signs, offset, local_width, 1)

    back_signs = lax.dynamic_slice_in_dim(signs, row_offset, own_rows, 1)[:, :, None]
    back_signs = jnp.broadcast_to(back_signs, (2, own_rows, cols))

    vmem = pl.BlockSpec(memory_space=pltpu.VMEM)
    bf16, f32 = jnp.bfloat16, jnp.float32
    pair = pltpu.SemaphoreType.DMA
    return pl.pallas_call(
        functools.partial(step_kernel, low_rows, chunk, token_count),
        out_shape=(
            jax.ShapeDtypeStruct((rows, local_width), bf16),
            jax.ShapeDtypeStruct((2, own, cols), f32),
            jax.ShapeDtypeStruct((2, own, cols), f32),
            jax.ShapeDtypeStruct((2, own_rows, cols), bf16),
        ),
        in_specs=[vmem] * 13,
        out_specs=(vmem,) * 4,
        scratch_shapes=[
            pltpu.VMEM((2, rows, rank), f32),
            pltpu.VMEM((n_tensor, 2, rows, cols), bf16),
            pltpu.VMEM((n_tensor - 1, rows, local_width), bf16),
            pltpu.VMEM((n_tensor - 1, rows, local_width), bf16),
            pltpu.VMEM((n_dp, n_tensor, 2, own, cols), bf16),
            pltpu.VMEM((n_dp - 1, n_tensor, 2, own, cols), bf16),
            pltpu.VMEM((n_tensor, 2, own, cols), f32),
            pltpu.VMEM((n_tensor, 2, own, cols), bf16),
            pltpu.VMEM((n_tensor - 1, 2, own, cols), bf16),
            pltpu.VMEM((n_dp, 2, own, cols), bf16),
            pltpu.VMEM((2, own_rows, rank), bf16),
            pair((2, n_tensor)),
            pair((2, n_tensor)),
            pair((2, n_dp)),
            pair((2, n_tensor)),
            pair((2, n_dp)),
        ],
        compiler_params=pltpu.CompilerParams(
            collective_id=0, has_side_effects=True, vmem_limit_bytes=56 * 1024 * 1024
        ),
    )(
        tokens, projection_weights, head_cotangent, my_signs, back_signs,
        ca, sa, cb, sb, ra, rb, first_moment, second_moment,
    )


def solution(mesh):
    in_specs = (
        P("dp", "tensor"),
        P(None, None, "tensor"),
        P(None, "dp", "tensor"),
        P(),
        P(),
        P(None, "dp", "tensor"),
        P(None, "dp", "tensor"),
    )
    out_specs = (
        P("dp", "tensor"),
        P(None, "dp", "tensor"),
        P(None, "dp", "tensor"),
        P(None, "dp", "tensor"),
    )
    return jax.shard_map(shards, mesh=mesh, in_specs=in_specs, out_specs=out_specs, check_vma=False)
```
